32 devices in a mesh: ma: 2 (over y), an: 4 (over z), ka: 4 (over x, core).
Axes of the slice: x: 2, y: 2, z: 4, core: 2. Of those that a mesh axis runs over, the one named last changes fastest.
Arguments:
- left_matrix: float32 [16384, 2048], P(('ka', 'an'), 'ma'), may hold values from -6 to 6
- right_matrix: float32 [16384, 3072], P(('ka', 'ma'), 'an'), may hold values from -0.046875 to 0.046875
Outputs:
- product: float32 [2048, 3072], P(('ma', 'ka'), 'an')
The draws below stay inside these ranges and needn't reach their ends.
All inputs are finite; a program needn't handle non-finite values.
Results may differ from the reference program's by a relative error of at most 0.000098.
Values sent between devices are 32-bit elements; how exact they have to be, the bound alone decides.
A program may use at most 128 MiB of HBM per device.

```python
import jax
import jax.numpy as jnp
from jax import lax

K = 16384
N = 3072
M = 2048


def with_spikes(drawn, key, source, target, parts, factor):
    def block_of(axis_at):
        return (jnp.arange(drawn.shape[axis_at]) // (drawn.shape[axis_at] // parts)).reshape((-1,) + (1,) * (drawn.ndim - 1 - axis_at))

    one_side = jax.random.permutation(key, parts)[block_of(target)]
    far = (block_of(target) + parts // 2) % parts
    return jnp.where((block_of(source) == one_side) | (block_of(source) == far), factor * drawn, drawn)


def level_of(own_key, dims, cuts, smallest, largest):
    gain = 1.0
    for axis_at, blocks in cuts:
        steps = jax.random.uniform(jax.random.fold_in(jax.random.fold_in(own_key, 6), axis_at), (blocks,), jnp.float32, smallest / len(cuts), largest / len(cuts))
        gain = gain * jnp.repeat(jnp.exp(steps), dims[axis_at] // blocks).reshape((-1,) + (1,) * (len(dims) - 1 - axis_at))
    return gain


def noise(rng, dims, scale, limit, shards=(), dtype=jnp.bfloat16):
    result = jax.random.normal(rng, dims, jnp.float32) * scale
    if len(shards) > 0:
        result = level_of(rng, dims, shards, -0.22, 0.18) * result
    return jnp.clip(result, min=-limit, max=limit).astype(dtype)


def noise_with(own_key, shape, spread, most, shards, heavy, dtype=jnp.bfloat16):
    values = spread * jax.random.normal(own_key, shape, jnp.float32)
    if shards:
        values = values * level_of(own_key, shape, shards, -0.22, 0.18)
    return jnp.clip(with_spikes(values, jax.random.fold_in(own_key, 3), *heavy), -most, most).astype(dtype)


def setup_inputs(seed: int = 0) -> dict:
    arg_keys = jax.random.split(jax.random.key(seed), 3)
    return {
        "left_matrix": noise_with(arg_keys[0], (K, M), 1.0, 6.0, ((0, 16), (1, 2)), (0, 1, 16, 2.0), jnp.float32),
        "right_matrix": noise(arg_keys[1], (K, N), K ** -0.5, 0.046875, ((0, 8), (1, 4)), jnp.float32),
    }


def reference(left_matrix, right_matrix):
    return lax.dot_general(left_matrix, right_matrix, (((0,), (0,)), ((), ())), precision=lax.Precision.HIGHEST, preferred_element_type=jnp.float32)
```

```python
import functools

import jax
import jax.numpy as jnp
from jax import lax
from jax.experimental import pallas as pl
from jax.experimental.pallas import tpu as pltpu
from jax.sharding import PartitionSpec as P

MESH = pl.DeviceIdType.MESH
PIECES = 4


def multiply(left_part, right_part):
    return lax.dot_general(
        left_part,
        right_part,
        (((0,), (0,)), ((), ())),
        precision=lax.Precision.HIGHEST,
        preferred_element_type=jnp.float32,
    )


def gather_both(left_matrix, right_matrix):
    b_block = lax.all_gather(right_matrix, "ma", axis=0, tiled=True)
    a_block = lax.all_gather(left_matrix, "an", axis=0, tiled=True)
    partial_value = multiply(a_block, b_block)
    return lax.psum_scatter(partial_value, "ka", scatter_dimension=0, tiled=True)


def halves(value):
    high = value.astype(jnp.bfloat16)
    low = (value - high.astype(jnp.float32)).astype(jnp.bfloat16)
    return high, low


def kernel(
    a_hbm, b_hbm, out,
    a_own, a_got, at_hi, at_lo, passing, b_got, b_hi, b_lo,
    part, core_got, x_got, z_got, y_sum, y_got,
    a_local, a_send, a_recv, pass_send, pass_recv, b_send, b_recv,
    core_send, core_recv, x_send, x_recv, z_send, z_recv, y_sem,
):
    ma, an, ka = lax.axis_index("ma"), lax.axis_index("an"), lax.axis_index("ka")
    x, core = ka // 2, lax.rem(ka, 2)
    other_y = 1 - ma
    over_core = x * 2 + (1 - core)
    over_x = (1 - x) * 2 + core
    depth, width = a_hbm.shape[0], b_got.shape[-1]
    rows = depth // PIECES
    band = a_own.shape[-1]

    def differs(one, two):
        return lax.rem(one // 2 + two // 2, 2) * 2 + lax.rem(one + two, 2)

    def at_distance(step):
        return lax.rem(an // 2 + step // 2, 2) * 2 + lax.rem(an + step, 2)

    def remote(source, target, send, recv, **where):
        return pltpu.make_async_remote_copy(
            src_ref=source, dst_ref=target, send_sem=send, recv_sem=recv,
            device_id=where, device_id_type=MESH,
        )

    barrier = pltpu.get_barrier_semaphore()
    peers = [{"ma": other_y}, {"ka": over_core}, {"ka": over_x}]
    peers += [{"an": at_distance(step)} for step in range(1, 4)]
    for peer in peers:
        pl.semaphore_signal(barrier, inc=1, device_id=peer, device_id_type=MESH)
    pl.semaphore_wait(barrier, len(peers))

    keep = pl.multiple_of(ma * width, 128)
    give = pl.multiple_of(other_y * width, 128)

    def pass_copy(which, piece):
        return remote(
            b_hbm.at[pl.ds(which * depth + piece * rows, rows), pl.ds(give, width)],
            passing.at[which, piece],
            pass_send.at[which, piece], pass_recv.at[which, piece], ma=other_y,
        )

    def a_copy(block):
        return remote(
            a_hbm.at[:, pl.ds(block * band, band)], a_got.at[block],
            a_send.at[block], a_recv.at[block], ma=other_y,
        )

    def own_copy(block):
        return pltpu.make_async_copy(
            a_hbm.at[:, pl.ds(block * band, band)], a_own.at[block], a_local.at[block]
        )

    def place(kind, which, piece):
        goal = (ma if kind == 0 else other_y) * 2 + which
        slot = differs(an, goal)
        if kind == 0:
            source = b_hbm.at[pl.ds(which * depth + piece * rows, rows), pl.ds(keep, width)]
        else:
            source = passing.at[which, piece]
        target = b_got.at[slot, piece]
        far = remote(
            source, target, b_send.at[kind, which, piece], b_recv.at[slot, piece], an=goal
        )
        near = pltpu.make_async_copy(source, target, b_recv.at[slot, piece])
        return goal, far, near

    def start_place(kind, which, piece):
        goal, far, near = place(kind, which, piece)

        @pl.when(goal != an)
        def _():
            far.start()

        @pl.when(goal == an)
        def _():
            near.start()

    for piece in range(PIECES):
        for which in range(2):
            pass_copy(which, piece).start()
            start_place(0, which, piece)
    for block in range(4):
        own_copy(block).start()
        a_copy(block).start()

    def turn(side, source, block):
        for cut in range(PIECES):
            span = pl.ds(cut * rows, rows)
            high, low = halves(source[block, span, :].T)
            at_hi[side, block, :, span] = high
            at_lo[side, block, :, span] = low

    for piece in range(PIECES):
        for which in range(2):
            pass_copy(which, piece).wait_recv()
            start_place(1, which, piece)
        own_copy(piece).wait()
        turn(0, a_own, piece)

    def b_wait(step):
        for piece in range(PIECES):
            pltpu.make_async_copy(
                passing.at[0, 0], b_got.at[step, piece], b_recv.at[step, piece]
            ).wait()

    def core_copy(unit, xo):
        return remote(
            part.at[unit, xo * 2 + (1 - core)], core_got.at[unit, xo],
            core_send.at[unit, xo], core_recv.at[unit, xo], ka=over_core,
        )

    def x_copy(unit):
        return remote(
            part.at[unit, over_x], x_got.at[unit], x_send.at[unit], x_recv.at[unit], ka=over_x
        )

    def z_copy(unit):
        side, step = unit // 4, unit % 4
        return remote(
            part.at[unit, ka], z_got.at[side, step - 1],
            z_send.at[unit], z_recv.at[side, step - 1], an=at_distance(step),
        )

    def compute(unit):
        side, step = unit // 4, unit % 4
        if side == 0:
            b_wait(step)
            for piece in range(PIECES):
                high, low = halves(b_got[step, piece])
                b_hi[step, pl.ds(piece * rows, rows), :] = high
                b_lo[step, pl.ds(piece * rows, rows), :] = low

        @pl.loop(0, 4)
        def _(block):
            dot = functools.partial(jnp.dot, preferred_element_type=jnp.float32)
            part[unit, block] = (
                dot(at_hi[side, block], b_lo[step]) + dot(at_lo[side, block], b_hi[step])
            ) + dot(at_hi[side, block], b_hi[step])

        for xo in range(2):
            core_copy(unit, xo).start()

    def add_core(unit):
        for xo in range(2):
            core_copy(unit, xo).wait_recv()
            part[unit, xo * 2 + core] += core_got[unit, xo]
        x_copy(unit).start()

    def add_x(unit):
        x_copy(unit).wait_recv()
        part[unit, ka] += x_got[unit]
        if unit % 4:
            z_copy(unit).start()

    def total(side):
        value = part[side * 4, ka]
        for step in range(1, 4):
            z_copy(side * 4 + step).wait_recv()
            value = value + z_got[side, step - 1]
        return value

    for unit in range(8):
        if unit == 4:
            for block in range(4):
                a_copy(block).wait_recv()
                turn(1, a_got, block)
        compute(unit)
        if unit >= 1:
            add_core(unit - 1)
        if unit >= 2:
            add_x(unit - 2)
    add_core(7)
    add_x(6)
    add_x(7)

    y_copy = remote(y_sum, y_got, y_sem.at[0], y_sem.at[1], ma=other_y)
    y_sum[...] = total(1)
    y_copy.start()
    out[:, pl.ds(keep, width)] = total(0)
    y_copy.wait_recv()
    out[:, pl.ds(give, width)] = y_got[...]

    y_copy.wait_send()
    for piece in range(PIECES):
        for which in range(2):
            pass_copy(which, piece).wait_send()
            for kind in range(2):
                goal, far, _ = place(kind, which, piece)

                @pl.when(goal != an)
                def _():
                    far.wait_send()

    for block in range(4):
        a_copy(block).wait_send()
    for unit in range(8):
        for xo in range(2):
            core_copy(unit, xo).wait_send()
        x_copy(unit).wait_send()
        if unit % 4:
            z_copy(unit).wait_send()


def exchange(left_matrix, right_matrix):
    depth, tall = left_matrix.shape
    width = right_matrix.shape[1] // 2
    band, rows = tall // 4, depth // PIECES
    f32, bf16, dma = jnp.float32, jnp.bfloat16, pltpu.SemaphoreType.DMA
    return pl.pallas_call(
        kernel,
        out_shape=jax.ShapeDtypeStruct((band, 2 * width), f32),
        in_specs=[pl.BlockSpec(memory_space=pl.ANY)] * 2,
        out_specs=pl.BlockSpec(memory_space=pltpu.VMEM),
        scratch_shapes=[
            pltpu.VMEM((4, depth, band), f32),
            pltpu.VMEM((4, depth, band), f32),
            pltpu.VMEM((2, 4, band, depth), bf16),
            pltpu.VMEM((2, 4, band, depth), bf16),
            pltpu.VMEM((2, PIECES, rows, width), f32),
            pltpu.VMEM((4, PIECES, rows, width), f32),
            pltpu.VMEM((4, depth, width), bf16),
            pltpu.VMEM((4, depth, width), bf16),
            pltpu.VMEM((8, 4, band, width), f32),
            pltpu.VMEM((8, 2, band, width), f32),
            pltpu.VMEM((8, band, width), f32),
            pltpu.VMEM((2, 3, band, width), f32),
            pltpu.VMEM((band, width), f32),
            pltpu.VMEM((band, width), f32),
            dma((4,)), dma((4,)), dma((4,)),
            dma((2, PIECES)), dma((2, PIECES)),
            dma((2, 2, PIECES)), dma((4, PIECES)),
            dma((8, 2)), dma((8, 2)), dma((8,)), dma((8,)),
            dma((8,)), dma((2, 3)), dma((2,)),
        ],
        compiler_params=pltpu.CompilerParams(
            collective_id=0, has_side_effects=True, vmem_limit_bytes=67043328
        ),
    )(left_matrix, right_matrix)


def fits(mesh, left, right):
    sizes = (mesh.shape["ma"], mesh.shape["an"], mesh.shape["ka"])
    if sizes != (2, 4, 4):
        return False
    depth, tall, width = left[0] // 16, left[1] // 2, right[1] // 8
    aligned = depth % 512 == 0 and tall % 512 == 0 and width % 128 == 0
    need = 4 * (3 * depth * tall + 9 * depth * width + 17 * tall * width)
    return aligned and need < 63 * 2**20


def solution(mesh):
    placed = (P(("ka", "an"), "ma"), P(("ka", "ma"), "an"))

    def run(left_matrix, right_matrix):
        body = exchange if fits(mesh, left_matrix.shape, right_matrix.shape) else gather_both
        return jax.shard_map(
            body, mesh=mesh, in_specs=placed, out_specs=P(("ma", "ka"), "an"), check_vma=False
        )(left_matrix, right_matrix)

    return run
```

```python
import functools

import jax
import jax.numpy as jnp
from jax import lax
from jax.experimental import pallas as pl
from jax.experimental.pallas import tpu as pltpu
from jax.sharding import PartitionSpec as P

MESH = pl.DeviceIdType.MESH
PIECES = 4


def multiply(left_part, right_part):
    return lax.dot_general(
        left_part,
        right_part,
        (((0,), (0,)), ((), ())),
        precision=lax.Precision.HIGHEST,
        preferred_element_type=jnp.float32,
    )


def gather_both(left_matrix, right_matrix):
    b_block = lax.all_gather(right_matrix, "ma", axis=0, tiled=True)
    a_block = lax.all_gather(left_matrix, "an", axis=0, tiled=True)
    partial_value = multiply(a_block, b_block)
    return lax.psum_scatter(partial_value, "ka", scatter_dimension=0, tiled=True)


def halves(value):
    high = value.astype(jnp.bfloat16)
    low = (value - high.astype(jnp.float32)).astype(jnp.bfloat16)
    return high, low


def kernel(
    a_hbm, b_hbm, out,
    a_own, a_got, at_hi, at_lo, passing, b_got, b_hi, b_lo,
    part, core_got, x_got, z_got, y_sum, y_got,
    a_local, a_send, a_recv, pass_send, pass_recv, b_send, b_recv,
    core_send, core_recv, x_send, x_recv, z_send, z_recv, y_sem,
):
    ma, an, ka = lax.axis_index("ma"), lax.axis_index("an"), lax.axis_index("ka")
    x, core = ka // 2, lax.rem(ka, 2)
    other_y = 1 - ma
    over_core = x * 2 + (1 - core)
    over_x = (1 - x) * 2 + core
    depth, width = a_hbm.shape[0], b_got.shape[-1]
    rows = depth // PIECES
    band = a_own.shape[-1]

    def differs(one, two):
        return lax.rem(one // 2 + two // 2, 2) * 2 + lax.rem(one + two, 2)

    def at_distance(step):
        return lax.rem(an // 2 + step // 2, 2) * 2 + lax.rem(an + step, 2)

    def remote(source, target, send, recv, **where):
        return pltpu.make_async_remote_copy(
            src_ref=source, dst_ref=target, send_sem=send, recv_sem=recv,
            device_id=where, device_id_type=MESH,
        )

    barrier = pltpu.get_barrier_semaphore()
    peers = [{"ma": other_y}, {"ka": over_core}, {"ka": over_x}]
    peers += [{"an": at_distance(step)} for step in range(1, 4)]
    for peer in peers:
        pl.semaphore_signal(barrier, inc=1, device_id=peer, device_id_type=MESH)
    pl.semaphore_wait(barrier, len(peers))

    keep = pl.multiple_of(ma * width, 128)
    give = pl.multiple_of(other_y * width, 128)
    sides_x = (1 - x, x)
    turns = [sides_x[order // 2] * 2 + lax.rem(1 - core + order, 2) for order in range(4)]
    goals = (lax.rem(an, 2), 1 - lax.rem(an, 2))

    def pass_copy(order, piece):
        return remote(
            b_hbm.at[pl.ds(goals[order] * depth + piece * rows, rows), pl.ds(give, width)],
            passing.at[order, piece],
            pass_send.at[order, piece], pass_recv.at[order, piece], ma=other_y,
        )

    def a_copy(order):
        columns = pl.ds(pl.multiple_of(turns[order] * band, 128), band)
        return remote(
            a_hbm.at[:, columns], a_got.at[order],
            a_send.at[order], a_recv.at[order], ma=other_y,
        )

    def own_copy(block):
        return pltpu.make_async_copy(
            a_hbm.at[:, pl.ds(block * band, band)], a_own.at[block], a_local.at[block]
        )

    def place(kind, order, piece):
        goal = (ma if kind == 0 else other_y) * 2 + goals[order]
        slot = differs(an, goal)
        if kind == 0:
            source = b_hbm.at[
                pl.ds(goals[order] * depth + piece * rows, rows), pl.ds(keep, width)
            ]
        else:
            source = passing.at[order, piece]
        target = b_got.at[slot, piece]
        far = remote(
            source, target, b_send.at[kind, order, piece], b_recv.at[slot, piece], an=goal
        )
        near = pltpu.make_async_copy(source, target, b_recv.at[slot, piece])
        return goal, far, near

    def start_place(kind, order, piece):
        goal, far, near = place(kind, order, piece)

        @pl.when(goal != an)
        def _():
            far.start()

        @pl.when(goal == an)
        def _():
            near.start()

    for order in range(2):
        for piece in range(PIECES):
            pass_copy(order, piece).start()
            start_place(0, order, piece)
    for block in range(4):
        own_copy(block).start()
        a_copy(block).start()

    def turn(side, source, held, block):
        for cut in range(PIECES):
            span = pl.ds(cut * rows, rows)
            high, low = halves(source[held, span, :].T)
            at_hi[side, block, :, span] = high
            at_lo[side, block, :, span] = low

    for order in range(2):
        for piece in range(PIECES):
            pass_copy(order, piece).wait_recv()
            start_place(1, order, piece)
            if piece % 2:
                block = order * 2 + piece // 2
                own_copy(block).wait()
                turn(0, a_own, block, block)

    def b_wait(step):
        for piece in range(PIECES):
            pltpu.make_async_copy(
                passing.at[0, 0], b_got.at[step, piece], b_recv.at[step, piece]
            ).wait()
            high, low = halves(b_got[step, piece])
            b_hi[step, pl.ds(piece * rows, rows), :] = high
            b_lo[step, pl.ds(piece * rows, rows), :] = low

    def core_copy(unit, near):
        return remote(
            part.at[unit, sides_x[near] * 2 + (1 - core)], core_got.at[unit, near],
            core_send.at[unit, near], core_recv.at[unit, near], ka=over_core,
        )

    def x_copy(unit):
        return remote(
            part.at[unit, over_x], x_got.at[unit], x_send.at[unit], x_recv.at[unit], ka=over_x
        )

    def z_copy(unit):
        side, step = unit // 4, unit % 4
        slot = {1: 0, 3: 1, 2: 2}[step]
        return remote(
            part.at[unit, ka], z_got.at[side, slot],
            z_send.at[side, slot], z_recv.at[side, slot], an=at_distance(2 if step == 2 else 1),
        )

    def compute(side, step, near):
        unit = side * 4 + step

        @pl.loop(0, 2)
        def _(turned):
            block = sides_x[near] * 2 + lax.rem(1 - core + turned, 2)
            dot = functools.partial(jnp.dot, preferred_element_type=jnp.float32)
            part[unit, block] = (
                dot(at_hi[side, block], b_lo[step]) + dot(at_lo[side, block], b_hi[step])
            ) + dot(at_hi[side, block], b_hi[step])

        core_copy(unit, near).start()

    def settle(side, step, near):
        unit = side * 4 + step
        core_copy(unit, near).wait_recv()
        if not near:
            part[unit, over_x] += core_got[unit, near]
            x_copy(unit).start()
            return
        x_copy(unit).wait_recv()
        part[unit, ka] += core_got[unit, near] + x_got[unit]
        if step % 2:
            z_copy(unit).start()

    def join_pairs(side):
        z_copy(side * 4 + 3).wait_recv()
        part[side * 4 + 2, ka] += z_got[side, 1]
        z_copy(side * 4 + 2).start()

    def total(side):
        z_copy(side * 4 + 1).wait_recv()
        value = part[side * 4, ka] + z_got[side, 0]
        z_copy(side * 4 + 2).wait_recv()
        return value + z_got[side, 2]

    def a_wait(order):
        a_copy(order).wait_recv()
        turn(1, a_got, order, turns[order])

    waiting = []

    def job(side, step, near):
        compute(side, step, near)
        if waiting:
            settle(*waiting.pop())
        waiting.append((side, step, near))

    for step in range(3):
        b_wait(step)
        job(0, step, 0)
        job(0, step, 1)
    for order in range(2):
        a_wait(order)
    for step in range(3):
        job(1, step, 0)
    b_wait(3)
    job(0, 3, 0)
    job(1, 3, 0)
    job(0, 3, 1)
    settle(*waiting.pop())
    for order in range(2, 4):
        a_wait(order)
    job(1, 3, 1)
    job(1, 1, 1)
    join_pairs(0)
    job(1, 2, 1)
    job(1, 0, 1)
    join_pairs(1)
    settle(*waiting.pop())

    y_copy = remote(y_sum, y_got, y_sem.at[0], y_sem.at[1], ma=other_y)
    y_sum[...] = total(1)
    y_copy.start()
    out[:, pl.ds(keep, width)] = total(0)
    y_copy.wait_recv()
    out[:, pl.ds(give, width)] = y_got[...]

    y_copy.wait_send()
    for order in range(2):
        for piece in range(PIECES):
            pass_copy(order, piece).wait_send()
            for kind in range(2):
                goal, far, _ = place(kind, order, piece)

                @pl.when(goal != an)
                def _():
                    far.wait_send()

    for order in range(4):
        a_copy(order).wait_send()
    for unit in range(8):
        for near in range(2):
            core_copy(unit, near).wait_send()
        x_copy(unit).wait_send()
        if unit % 4:
            z_copy(unit).wait_send()


def exchange(left_matrix, right_matrix):
    depth, tall = left_matrix.shape
    width = right_matrix.shape[1] // 2
    band, rows = tall // 4, depth // PIECES
    f32, bf16, dma = jnp.float32, jnp.bfloat16, pltpu.SemaphoreType.DMA
    return pl.pallas_call(
        kernel,
        out_shape=jax.ShapeDtypeStruct((band, 2 * width), f32),
        in_specs=[pl.BlockSpec(memory_space=pl.ANY)] * 2,
        out_specs=pl.BlockSpec(memory_space=pltpu.VMEM),
        scratch_shapes=[
            pltpu.VMEM((4, depth, band), f32),
            pltpu.VMEM((4, depth, band), f32),
            pltpu.VMEM((2, 4, band, depth), bf16),
            pltpu.VMEM((2, 4, band, depth), bf16),
            pltpu.VMEM((2, PIECES, rows, width), f32),
            pltpu.VMEM((4, PIECES, rows, width), f32),
            pltpu.VMEM((4, depth, width), bf16),
            pltpu.VMEM((4, depth, width), bf16),
            pltpu.VMEM((8, 4, band, width), f32),
            pltpu.VMEM((8, 2, band, width), f32),
            pltpu.VMEM((8, band, width), f32),
            pltpu.VMEM((2, 3, band, width), f32),
            pltpu.VMEM((band, width), f32),
            pltpu.VMEM((band, width), f32),
            dma((4,)), dma((4,)), dma((4,)),
            dma((2, PIECES)), dma((2, PIECES)),
            dma((2, 2, PIECES)), dma((4, PIECES)),
            dma((8, 2)), dma((8, 2)), dma((8,)), dma((8,)),
            dma((2, 3)), dma((2, 3)), dma((2,)),
        ],
        compiler_params=pltpu.CompilerParams(
            collective_id=0, has_side_effects=True, vmem_limit_bytes=67043328
        ),
    )(left_matrix, right_matrix)


def fits(mesh, left, right):
    sizes = (mesh.shape["ma"], mesh.shape["an"], mesh.shape["ka"])
    if sizes != (2, 4, 4):
        return False
    depth, tall, width = left[0] // 16, left[1] // 2, right[1] // 8
    aligned = depth % 512 == 0 and tall % 512 == 0 and width % 128 == 0
    need = 4 * (3 * depth * tall + 9 * depth * width + 17 * tall * width)
    return aligned and need < 63 * 2**20


def solution(mesh):
    placed = (P(("ka", "an"), "ma"), P(("ka", "ma"), "an"))

    def run(left_matrix, right_matrix):
        body = exchange if fits(mesh, left_matrix.shape, right_matrix.shape) else gather_both
        return jax.shard_map(
            body, mesh=mesh, in_specs=placed, out_specs=P(("ma", "ka"), "an"), check_vma=False
        )(left_matrix, right_matrix)

    return run
```
